256 devices in a mesh: blk: 32 (over y_lo, z, core), col: 8 (over y_hi, x).
Axes of the slice: x: 4, y: 4 (y_hi: 2, y_lo: 2; y = y_hi * 2 + y_lo), z: 8, core: 2. Of those that a mesh axis runs over, the one named last changes fastest.
Arguments:
- counts: float32 [8192, 8192], P('blk', 'col'), may hold values from 0.1 to 10
- merge_map: int32 [8192, 1], replicated, may hold values from 0 to 4095, as said below
Outputs:
- merged: float32 [4096, 4096], P('blk', 'col')
- block_terms: float32 [4096], P('blk')
The draws below stay inside these ranges and needn't reach their ends.
Inputs may be any that keep to these rules, and one draw needn't show every extreme that they name: `merge_map`: every new block is the image of exactly two old blocks. Let the owner of new block r be r // 128. The 256 old blocks i with i // 256 = s, for each s, map to new blocks of exactly 16 distinct owners, exactly 16 old blocks to each of them, and each owner receives from exactly 16 such s.
All inputs are finite; a program needn't handle non-finite values.
Results may differ from the reference program's by a relative error of at most 0.0003.
Values sent between devices are 32-bit elements; how exact they have to be, the bound alone decides.
A program may use at most 64 MiB of HBM per device.

```python
import math
import jax
import jax.numpy as jnp

B = 8192
NB = 4096
ROWS_DEV = 256
OWNED_DEV = 128
FANOUT = 16
SLOT_CAP = 16
N_BLK = 32


def draw_merge_map(key, part):
    base = jax.random.fold_in(key, 11)
    key_src, key_off, key_row, key_slot = jax.random.split(base, 4)
    placing = jax.random.permutation(key_src, N_BLK)
    offsets = jax.random.permutation(key_off, N_BLK)[:FANOUT]
    row_keys = jax.random.split(key_row, N_BLK)
    ranking = jax.vmap(lambda single: jax.random.permutation(single, ROWS_DEV))(row_keys)
    group = ranking // SLOT_CAP
    within = ranking % SLOT_CAP
    owner = (placing[:, None] + offsets[group]) % N_BLK
    slot_keys = jax.random.split(key_slot, N_BLK)
    shuffles = jax.vmap(lambda single: jax.random.permutation(single, ROWS_DEV))(slot_keys)
    placed = shuffles[owner, group * SLOT_CAP + within]
    new_ids = owner * OWNED_DEV + placed // 2
    return new_ids.reshape(B, 1).astype(jnp.int32)


def block_scale(key, shape, shards, low, largest):
    def one(dim, blocks):
        heights = jax.random.uniform(jax.random.fold_in(jax.random.fold_in(key, 6), dim), (blocks,), jnp.float32, low / len(shards), largest / len(shards))
        return jnp.repeat(jnp.exp(heights), shape[dim] // blocks).reshape((-1,) + (1,) * (len(shape) - dim - 1))

    factor_of = one(*shards[0])
    for cut in shards[1:]:
        factor_of = factor_of * one(*cut)
    return factor_of


def setup_inputs(seed: int = 0) -> dict:
    splits = jax.random.split(jax.random.key(seed), 3)
    counts = jnp.clip(jnp.exp(math.log(10.0) - 4.6051702 * jax.random.uniform(splits[0], (B, B), jnp.float32) ** block_scale(splits[0], (B, B), ((0, 32), (1, 8)), -0.2, 0.2)), 0.1, 10.0)
    merge_map = draw_merge_map(jax.random.fold_in(splits[2], 71), 0)
    return {"counts": counts, "merge_map": merge_map}


def reference(counts, merge_map):
    ids = merge_map[:, 0].astype(jnp.int32)
    rows = jax.ops.segment_sum(counts, ids, num_segments=NB)
    merged = jax.ops.segment_sum(rows.T, ids, num_segments=NB).T
    out_total = jnp.sum(merged, axis=1)
    in_total = jnp.sum(merged, axis=0)
    total = jnp.sum(in_total)
    share = merged / out_total[:, None]
    ratio = merged * total / (out_total[:, None] * in_total[None, :])
    block_terms = jnp.sum(share * jnp.log(ratio), axis=1)
    return merged, block_terms
```

```python
import jax
import jax.numpy as jnp
from jax import lax
from jax.experimental import pallas as pl
from jax.experimental.pallas import tpu as pltpu
from jax.sharding import PartitionSpec as P

MESH = pl.DeviceIdType.MESH
F32 = jnp.float32
BF16 = jnp.bfloat16
I32 = jnp.int32
NQ = 4
NB_PEERS = 31


def split(v):
    high = v.astype(BF16)
    return high, (v - high.astype(F32)).astype(BF16)


def dot_nn(a, b):
    return lax.dot_general(a, b, (((1,), (0,)), ((), ())), preferred_element_type=F32)


def dot_nt(a, b):
    return lax.dot_general(a, b, (((1,), (1,)), ((), ())), preferred_element_type=F32)


def iota(shape, dim):
    return lax.broadcasted_iota(I32, shape, dim)


def one_hot(mask):
    return jnp.where(mask, 1.0, 0.0).astype(BF16)


def slot_keys(rows):
    owners = [lax.shift_right_logical(r, 7) for r in rows]
    hits = [o == iota((32, 256), 0) for o in owners]
    table = jnp.concatenate([jnp.where(h, 1.0, 0.0) for h in hits], axis=0)
    before = one_hot(iota((256, 256), 0) < iota((256, 256), 1))
    counted = dot_nn(table.astype(BF16), before) * table
    ranks = [
        jnp.sum(counted[i * 32 : (i + 1) * 32], axis=0, keepdims=True).astype(I32)
        for i in range(len(rows))
    ]
    return [o * 16 + r for o, r in zip(owners, ranks)]


def kernel(
    counts_hbm,
    ids,
    merged,
    terms,
    counts,
    parts,
    keys,
    coltag,
    rowtag,
    unpack_rows,
    pack_rows,
    mine,
    xsend,
    xrecv,
    ysend,
    yrecv,
    zsend,
    zrecv,
    csend,
    crecv,
    tsend,
    trecv,
    in_sem,
    xs,
    xr,
    ys,
    yr,
    zs,
    zr,
    cs,
    cr,
    ts,
    tr,
):
    b = lax.axis_index("blk")
    c = lax.axis_index("col")
    x = c % 4
    yh = c // 4

    load = pltpu.make_async_copy(counts_hbm, counts, in_sem)
    load.start()

    barrier = pltpu.get_barrier_semaphore()

    def greet(t, carry):
        pl.semaphore_signal(barrier, inc=1, device_id=((b + t) % 32, c), device_id_type=MESH)
        return carry

    lax.fori_loop(1, 32, greet, 0)
    for t in range(1, 8):
        pl.semaphore_signal(barrier, inc=1, device_id=(b, (c + t) % 8), device_id_type=MESH)

    positions = []
    for g, key in enumerate(slot_keys([ids[c * 4 + g] for g in range(4)])):
        owner = lax.shift_right_logical(key, 4)
        to = lax.shift_right_logical(owner, 2)
        dx = (to - x) & 3
        tile = jnp.where(dx == 2, 0, jnp.where(dx == 1, 1, jnp.where(dx == 3, 2, 3)))
        half = (lax.shift_right_logical(to, 2) - yh) & 1
        positions.append((owner & 3) * 512 + tile * 128 + half * 64 + g * 16 + (key & 15))
    position = jnp.concatenate(positions, axis=1)

    load.wait()
    high, low = split(counts[...])
    parts[0] = high
    parts[1] = low
    pl.semaphore_wait(barrier, 38)

    def x_copy(q, dx):
        return pltpu.make_async_remote_copy(
            src_ref=xsend.at[q, dx],
            dst_ref=xrecv.at[q, dx],
            send_sem=xs.at[q, dx],
            recv_sem=xr.at[q, dx],
            device_id=(b, yh * 4 + (x + dx) % 4),
            device_id_type=MESH,
        )

    def pack(q, carry):
        for first, tiles in ((0, (2, 1)), (256, (3, 0))):
            pick = one_hot(position - q * 512 == iota((256, 1024), 0) + first)
            packed = dot_nt(parts[0], pick) + dot_nt(parts[1], pick)
            for i, dx in enumerate(tiles):
                value = packed[:, i * 128 : (i + 1) * 128]
                if dx == 0:
                    xrecv[q, 0] = value
                else:
                    xsend[q, dx] = value
                    x_copy(q, dx).start()
        return carry

    lax.fori_loop(0, NQ, pack, 0)

    def all_keys(i, carry):
        for g, key in enumerate(slot_keys([ids[i * 4 + g] for g in range(4)])):
            keys[i * 4 + g] = key
        return carry

    lax.fori_loop(0, 8, all_keys, 0)

    slot = iota((128, 1), 0)
    half = lax.shift_right_logical(slot, 4) & 1
    wanted = (((half ^ yh) * 4 + x) * 4 + lax.shift_right_logical(slot, 5)) * 16 + (slot & 15)

    def column_tags(i, carry):
        dx, g = i // 4, i % 4
        s = yh * 16 + ((x + 4 - dx) % 4) * 4 + g
        value = (ids[s] & 127) + 1 + half * 128
        tag = jnp.sum(jnp.where(keys[s] == wanted, value, 0).astype(F32), axis=1, keepdims=True)
        for q in range(NQ):
            for p in range(2):
                coltag[q, dx, p, g] = tag[(q * 2 + p) * 16 : (q * 2 + p + 1) * 16]
        return carry

    lax.fori_loop(0, 16, column_tags, 0)

    def row_tags(s, carry):
        value = (ids[s] & 127) + 1
        hit = keys[s] == b * 16 + iota((16, 1), 0)
        rowtag[s] = jnp.sum(jnp.where(hit, value, 0).astype(F32), axis=1, keepdims=True)
        return carry

    lax.fori_loop(0, 32, row_tags, 0)
    flat = rowtag[...].reshape(512, 1).astype(I32)
    unpack_rows[...] = jnp.where(flat == iota((512, 128), 1) + 1, 1.0, 0.0).T.astype(BF16)
    pack_rows[...] = one_hot(keys[b] == iota((512, 256), 0))

    def y_copy(q):
        return pltpu.make_async_remote_copy(
            src_ref=ysend.at[q],
            dst_ref=yrecv.at[q],
            send_sem=ys.at[q],
            recv_sem=yr.at[q],
            device_id=(b, (c + 4) % 8),
            device_id_type=MESH,
        )

    def after_x(q):
        for dx in range(1, 4):
            x_copy(q, dx).wait_recv()
        tag = coltag[q].reshape(512, 1).astype(I32)
        place = one_hot(tag == iota((512, 256), 1) + 1)
        got = jnp.concatenate([xrecv[q, dx] for dx in range(4)], axis=1)
        high, low = split(got)
        both = dot_nn(high, place) + dot_nn(low, place)
        ysend[q] = both[:, 128:]
        y_copy(q).start()
        mine[q] = both[:, :128]

    def z_copy(q, t):
        core = t % 2
        y = (t // 2) % 2
        i = 7 - t // 4
        z = (i % 2) * ((i + 1) // 2) + (1 - i % 2) * (8 - i // 2)
        zb = (b // 2 + z) % 8
        d = (((b // 16) + y) % 2 * 8 + zb) * 2 + (b + core) % 2
        rows = pltpu.make_async_remote_copy(
            src_ref=zsend.at[q, d],
            dst_ref=zrecv.at[q, b],
            send_sem=zs.at[q],
            recv_sem=zr.at[q],
            device_id=(d, c),
            device_id_type=MESH,
        )
        sums = pltpu.make_async_remote_copy(
            src_ref=csend.at[q],
            dst_ref=crecv.at[q, b],
            send_sem=cs.at[q],
            recv_sem=cr.at[q],
            device_id=(d, c),
            device_id_type=MESH,
        )
        return rows, sums

    def z_all(q, s_ref, r_ref, s_sem, r_sem):
        return pltpu.make_async_remote_copy(
            src_ref=s_ref.at[q, pl.ds(0, NB_PEERS)],
            dst_ref=r_ref.at[q, pl.ds(0, NB_PEERS)],
            send_sem=s_sem.at[q],
            recv_sem=r_sem.at[q],
            device_id=((b + 1) % 32, c),
            device_id_type=MESH,
        )

    def after_y(q):
        y_copy(q).wait_recv()
        block = mine[q] + yrecv[q]
        sums = jnp.sum(block, axis=0, keepdims=True)
        csend[q] = sums
        crecv[q, b] = sums
        high, low = split(block)
        packed = dot_nn(pack_rows[...], high) + dot_nn(pack_rows[...], low)
        zsend[q] = packed.reshape(32, 16, 128)
        zrecv[q, b] = zsend[q, b]

        def send(t, carry):
            rows, sums = z_copy(q, t)
            rows.start()
            sums.start()
            return carry

        lax.fori_loop(0, 28, send, 0)
        lax.fori_loop(29, 32, send, 0)

    weighted, row_sum, col_sum = [], [], []

    def after_z(q):
        z_all(q, zsend, zrecv, zs, zr).wait_recv()
        z_all(q, crecv, crecv, cs, cr).wait_recv()
        high, low = split(zrecv[q].reshape(512, 128))
        out = dot_nn(unpack_rows[...], high) + dot_nn(unpack_rows[...], low)
        merged[:, q * 128 : (q + 1) * 128] = out
        arriving = jnp.sum(crecv[q], axis=0)
        weighted.append(out * (jnp.log(out * 0.25) - jnp.log(arriving * (2.0**-14))))
        row_sum.append(out)
        col_sum.append(arriving)

    for step in range(NQ + 2):
        if step < NQ:
            after_x(step)
        if 0 <= step - 1 < NQ:
            after_y(step - 1)
        if 0 <= step - 2:
            after_z(step - 2)

    tsend[0:1] = jnp.sum(sum(weighted).T, axis=0, keepdims=True)
    tsend[1:2] = jnp.sum(sum(row_sum).T, axis=0, keepdims=True)
    tsend[2:3] = sum(col_sum)
    tsend[3:8] = jnp.zeros((5, 128), F32)
    trecv[0] = tsend[...]

    def t_copy(t):
        return pltpu.make_async_remote_copy(
            src_ref=tsend,
            dst_ref=trecv.at[t],
            send_sem=ts.at[t],
            recv_sem=tr.at[t],
            device_id=(b, (c + t) % 8),
            device_id_type=MESH,
        )

    for t in range(1, 8):
        t_copy(t).start()
    for t in range(1, 8):
        t_copy(t).wait_recv()
    everyone = jnp.sum(trecv[...], axis=0)
    out_total = everyone[1:2]
    total = jnp.sum(everyone[2:3], axis=1, keepdims=True)
    terms[...] = (
        everyone[0:1] / out_total
        + jnp.log(total * (2.0**-26))
        - jnp.log(out_total * (2.0**-14))
    )

    for q in range(NQ):
        for dx in range(1, 4):
            x_copy(q, dx).wait_send()
        y_copy(q).wait_send()
        z_all(q, zsend, zrecv, zs, zr).wait_send()
        z_all(q, crecv, crecv, cs, cr).wait_send()
    for t in range(1, 8):
        t_copy(t).wait_send()


def shards(counts, merge_map):
    ids = merge_map.reshape(32, 1, 256)
    dma = pltpu.SemaphoreType.DMA
    merged, terms = pl.pallas_call(
        kernel,
        out_shape=(
            jax.ShapeDtypeStruct((128, 512), F32),
            jax.ShapeDtypeStruct((1, 128), F32),
        ),
        in_specs=[
            pl.BlockSpec(memory_space=pl.ANY),
            pl.BlockSpec(memory_space=pltpu.VMEM),
        ],
        out_specs=(
            pl.BlockSpec(memory_space=pltpu.VMEM),
            pl.BlockSpec(memory_space=pltpu.VMEM),
        ),
        scratch_shapes=[
            pltpu.VMEM((256, 1024), F32),
            pltpu.VMEM((2, 256, 1024), BF16),
            pltpu.VMEM((32, 1, 256), I32),
            pltpu.VMEM((NQ, 4, 2, 4, 16, 1), F32),
            pltpu.VMEM((32, 16, 1), F32),
            pltpu.VMEM((128, 512), BF16),
            pltpu.VMEM((512, 256), BF16),
            pltpu.VMEM((NQ, 256, 128), F32),
            pltpu.VMEM((NQ, 4, 256, 128), F32),
            pltpu.VMEM((NQ, 4, 256, 128), F32),
            pltpu.VMEM((NQ, 256, 128), F32),
            pltpu.VMEM((NQ, 256, 128), F32),
            pltpu.VMEM((NQ, 32, 16, 128), F32),
            pltpu.VMEM((NQ, 32, 16, 128), F32),
            pltpu.VMEM((NQ, 1, 128), F32),
            pltpu.VMEM((NQ, 32, 1, 128), F32),
            pltpu.VMEM((8, 128), F32),
            pltpu.VMEM((8, 8, 128), F32),
            dma,
            dma((NQ, 4)),
            dma((NQ, 4)),
            dma((NQ,)),
            dma((NQ,)),
            dma((NQ,)),
            dma((NQ,)),
            dma((NQ,)),
            dma((NQ,)),
            dma((8,)),
            dma((8,)),
        ],
        compiler_params=pltpu.CompilerParams(
            collective_id=0, has_side_effects=True, vmem_limit_bytes=48 * 1024 * 1024
        ),
    )(counts, ids)
    return merged, terms.reshape(128)


def solution(mesh):
    return jax.shard_map(
        shards,
        mesh=mesh,
        in_specs=(P("blk", "col"), P()),
        out_specs=(P("blk", "col"), P("blk")),
        check_vma=False,
    )
```

```python
import jax
import jax.numpy as jnp
from jax import lax
from jax.experimental import pallas as pl
from jax.experimental.pallas import tpu as pltpu
from jax.sharding import PartitionSpec as P

MESH = pl.DeviceIdType.MESH
F32 = jnp.float32
BF16 = jnp.bfloat16
I32 = jnp.int32
NQ = 4
NP = 4
Z_STEPS = (4, 3, 5, 0, 2, 6, 1, 7)
DIRECT = ()
RELAYED = (0, 1, 2, 3)
ND, NR = len(DIRECT), len(RELAYED)
ORDER = (
    "tokens",
    "p2",
    "x0",
    "p3",
    "tags",
    "a0",
    "x1",
    "b0",
    "c0",
    "d0",
    "x2",
    "a1",
    "b1",
    "c1",
    "d1",
    "z0",
    "x3",
    "a2",
    "b2",
    "c2",
    "d2",
    "z1",
    "a3",
    "b3",
    "c3",
    "d3",
    "z2",
    "z3",
)


def split(v):
    high = v.astype(BF16)
    return high, (v - high.astype(F32)).astype(BF16)


def dot_nn(a, b):
    return lax.dot_general(a, b, (((1,), (0,)), ((), ())), preferred_element_type=F32)


def dot_nt(a, b):
    return lax.dot_general(a, b, (((1,), (1,)), ((), ())), preferred_element_type=F32)


def iota(shape, dim):
    return lax.broadcasted_iota(I32, shape, dim)


def one_hot(mask):
    return jnp.where(mask, 1.0, 0.0).astype(BF16)


def slot_keys(rows):
    owners = [lax.shift_right_logical(r, 7) for r in rows]
    hits = [o == iota((32, 256), 0) for o in owners]
    table = jnp.concatenate([jnp.where(h, 1.0, 0.0) for h in hits], axis=0)
    before = one_hot(iota((256, 256), 0) < iota((256, 256), 1))
    counted = dot_nn(table.astype(BF16), before) * table
    ranks = [
        jnp.sum(counted[i * 32 : (i + 1) * 32], axis=0, keepdims=True).astype(I32)
        for i in range(len(rows))
    ]
    return [o * 16 + r for o, r in zip(owners, ranks)]


def kernel(
    counts_hbm,
    ids_hbm,
    merged,
    terms,
    counts,
    ids,
    parts,
    keys,
    nearby,
    coltag,
    rowtag,
    unpack_rows,
    pack_rows,
    dsend,
    drecv,
    xsend,
    xrecv,
    asend,
    arecv,
    bsend,
    brecv,
    zsend,
    zrecv,
    csend,
    crecv,
    tsend,
    trecv,
    in_sem,
    ids_sem,
    ds,
    dr,
    xs,
    xr,
    ys,
    yr,
    zs,
    zr,
    cs,
    cr,
    ts,
    tr,
    token,
):
    b = lax.axis_index("blk")
    c = lax.axis_index("col")
    x, yh = lax.rem(c, 4), lax.div(c, 4)
    core, zz, yl = lax.rem(b, 2), lax.rem(lax.div(b, 2), 8), lax.div(b, 16)

    ids_load = pltpu.make_async_copy(ids_hbm, ids, ids_sem)
    ids_load.start()
    load = pltpu.make_async_copy(counts_hbm, counts, in_sem)
    load.start()

    barrier = pltpu.get_barrier_semaphore()

    def z_peer(step, k):
        return (yl * 8 + lax.rem(zz + step, 8)) * 2 + lax.rem(core + k, 2)

    def y_peer(p, r):
        return lax.rem(yl + r, 2) * 16 + zz * 2 + core, lax.rem(c + 4 * p, 8)

    def greet(peer):
        pl.semaphore_signal(barrier, inc=1, device_id=peer, device_id_type=MESH)

    for dx in range(1, 4):
        greet((b, yh * 4 + lax.rem(x + dx, 4)))
    for p, r in ((1, 0), (0, 1), (1, 1)):
        greet(y_peer(p, r))
    for step, k in ((1, 0), (7, 0), (0, 1)):
        greet((z_peer(step, k), c))

    ids_load.wait()
    positions = []
    for g, key in enumerate(slot_keys([ids[c * 4 + g] for g in range(4)])):
        owner = lax.shift_right_logical(key, 4)
        to = lax.shift_right_logical(owner, 2)
        dx = (to - x) & 3
        tile = jnp.where(dx == 2, 0, jnp.where(dx == 1, 1, jnp.where(dx == 3, 2, 3)))
        half = (lax.shift_right_logical(to, 2) - yh) & 1
        positions.append((owner & 3) * 512 + tile * 128 + half * 64 + g * 16 + (key & 15))
    position = jnp.concatenate(positions, axis=1)

    load.wait()
    high, low = split(counts[...])
    parts[0] = high
    parts[1] = low

    def x_copy(q, dx):
        return pltpu.make_async_remote_copy(
            src_ref=xsend.at[q, dx],
            dst_ref=xrecv.at[q, dx],
            send_sem=xs.at[q, dx],
            recv_sem=xr.at[q, dx],
            device_id=(b, yh * 4 + lax.rem(x + dx, 4)),
            device_id_type=MESH,
        )

    def d_copy(q, p, dx):
        return pltpu.make_async_remote_copy(
            src_ref=dsend.at[q, p, dx],
            dst_ref=drecv.at[q, p, dx],
            send_sem=ds.at[q, p, dx],
            recv_sem=dr.at[q, p, dx],
            device_id=(b, lax.rem(yh + p, 2) * 4 + lax.rem(x + dx, 4)),
            device_id_type=MESH,
        )

    first_half = iota((128, 128), 1) < 64

    def pack(q):
        for first, tiles in ((0, (2, 1)), (256, (3, 0))):
            pick = one_hot(position - q * 512 == iota((256, 1024), 0) + first)
            packed = dot_nt(parts[0], pick) + dot_nt(parts[1], pick)
            for i, dx in enumerate(tiles):
                value = packed[:, i * 128 : (i + 1) * 128]
                if q in DIRECT:
                    at = DIRECT.index(q)
                    top, bottom = value[:128], value[128:]
                    for p in (1, 0):
                        if p:
                            both = jnp.where(first_half, pltpu.roll(top, 64, 1), bottom)
                        else:
                            both = jnp.where(first_half, top, pltpu.roll(bottom, 64, 1))
                        if p == 0 and dx == 0:
                            drecv[at, 0, 0] = both
                        else:
                            dsend[at, p, dx] = both
                else:
                    at = RELAYED.index(q)
                    if dx == 0:
                        xrecv[at, 0] = value
                    else:
                        xsend[at, dx] = value
            if q > 0:
                send_columns(q, tiles)

    def send_columns(q, tiles):
        for dx in tiles:
            if q in DIRECT:
                for p in (1, 0):
                    if p or dx:
                        d_copy(DIRECT.index(q), p, dx).start()
            elif dx:
                x_copy(RELAYED.index(q), dx).start()


    sixteen = iota((16, 1), 0)

    def pass_token(i):
        for way, step in enumerate((1, 7)):
            pl.semaphore_signal(
                token.at[i, way], inc=1, device_id=(z_peer(step, 0), c), device_id_type=MESH
            )

    def take_token(i):
        for way in range(2):
            pl.semaphore_wait(token.at[i, way], 1)


    def all_keys():
        for i in range(4):
            for g, key in enumerate(slot_keys([ids[i * 8 + g] for g in range(8)])):
                keys[i * 8 + g] = key

    def column_tags():
        near = [c * 4 + q for q in DIRECT]
        far = [(lax.rem(yh + p, 2) * 4 + x) * 4 + q for q in RELAYED for p in range(2)]
        for p in range(2):
            owners = near + far if p == 0 else near
            if not owners:
                continue
            wanted = jnp.concatenate([o * 16 + sixteen for o in owners], axis=0)
            for dx in range(4):
                for g in range(4):
                    src = lax.rem(yh + p, 2) * 16 + lax.rem(x + 4 - dx, 4) * 4 + g
                    value = ((ids[src] & 127) + 1).astype(F32)
                    tag = jnp.sum(
                        jnp.where(keys[src] == wanted, value, 0.0), axis=1, keepdims=True
                    )
                    other = jnp.where(tag > 0.0, tag + 128.0, 0.0)
                    for i in range(ND):
                        nearby[i, p, dx, 0, g] = tag[i * 16 : i * 16 + 16]
                        nearby[i, p, dx, 1, g] = other[i * 16 : i * 16 + 16]
                    if p == 0:
                        for i in range(NR):
                            at = ND * 16 + i * 32
                            coltag[i, dx, 0, g] = tag[at : at + 16]
                            coltag[i, dx, 1, g] = other[at + 16 : at + 32]

    def row_places():
        key = keys[b]
        owner = lax.shift_right_logical(key, 4)
        k = (owner - core) & 1
        dz = (lax.shift_right_logical(owner, 1) - zz) & 7
        r = (lax.shift_right_logical(owner, 4) - yl) & 1
        at = sum(jnp.where(dz == step, i, 0) for i, step in enumerate(Z_STEPS))
        place = (at >> 1) * 128 + r * 64 + (at & 1) * 32 + k * 16 + (key & 15)
        pack_rows[...] = one_hot(place == iota((512, 256), 0))

    def row_tags():
        for i, step in enumerate(Z_STEPS):
            for k in range(2):
                for r in range(2):
                    z = lax.rem(zz + 8 - step, 8)
                    src = (lax.rem(yl + r, 2) * 8 + z) * 2 + lax.rem(core + k, 2)
                    value = ((ids[src] & 127) + 1).astype(F32)
                    hit = keys[src] == b * 16 + sixteen
                    rowtag[(i * 2 + k) * 2 + r] = jnp.sum(
                        jnp.where(hit, value, 0.0), axis=1, keepdims=True
                    )
        flat = rowtag[...].reshape(512, 1).astype(I32)
        unpack_rows[...] = jnp.where(flat == iota((512, 128), 1) + 1, 1.0, 0.0).T.astype(BF16)

    pack(0)
    pl.semaphore_wait(barrier, 9)
    send_columns(0, (2, 1, 3, 0))
    pass_token(0)
    pack(1)
    all_keys()
    column_tags()
    row_places()

    def y_peers(q):
        return ((0, 1),) if q in DIRECT else ((1, 0), (1, 1), (0, 1))

    def y_refs(q, part):
        if part == 0:
            return asend.at[q], arecv.at[q]
        return bsend.at[q, part - 1], brecv.at[q, part - 1]

    def y_copy(q, part, p, r):
        src, dst = y_refs(q, part)
        return pltpu.make_async_remote_copy(
            src_ref=src.at[p, r],
            dst_ref=dst.at[p, r],
            send_sem=ys.at[q, part, p, r],
            recv_sem=yr.at[q, part, p, r],
            device_id=y_peer(p, r),
            device_id_type=MESH,
        )

    def after_x(q):
        i = RELAYED.index(q)
        tag = coltag[i].reshape(512, 1).astype(I32)
        place = one_hot(tag == iota((512, 256), 1) + 1)
        for dx in range(1, 4):
            x_copy(i, dx).wait_recv()
        got = jnp.concatenate([xrecv[i, dx] for dx in range(4)], axis=1)
        high, low = split(got)
        send_y(q, dot_nn(high, place) + dot_nn(low, place), 2)

    def after_d(q):
        i = DIRECT.index(q)
        tag = nearby[i].reshape(1024, 1).astype(I32)
        place = one_hot(tag == iota((1024, 256), 1) + 1)
        for p in range(2):
            for dx in range(4):
                if p or dx:
                    d_copy(i, p, dx).wait_recv()
        got = jnp.concatenate([drecv[i, p, dx] for p in range(2) for dx in range(4)], axis=1)
        high, low = split(got)
        both = dot_nn(high, place) + dot_nn(low, place)
        send_y(q, jnp.concatenate([both[:, :128], both[:, 128:]], axis=0), 1)

    def send_y(q, block, halves):
        sums = jnp.sum(block, axis=0, keepdims=True)
        high, low = split(block)
        for part in range(NP):
            pick = pack_rows[part * 128 : (part + 1) * 128]
            packed = dot_nn(pick, high) + dot_nn(pick, low)
            out = y_refs(q, part)[0]
            for p in range(halves):
                for r in range(2):
                    at = r * 64
                    out[p, r, 0:64] = packed[at : at + 64, p * 128 : (p + 1) * 128]
                    if part == 0:
                        out[p, r, 64:72] = jnp.broadcast_to(
                            sums[:, p * 128 : (p + 1) * 128], (8, 128)
                        )
            for p, r in y_peers(q):
                y_copy(q, part, p, r).start()

    def to_z(step, k, src, dst, send, recv):
        return pltpu.make_async_remote_copy(
            src_ref=src,
            dst_ref=dst,
            send_sem=send,
            recv_sem=recv,
            device_id=(z_peer(step, k), c),
            device_id_type=MESH,
        )

    def all_rows(q, part):
        few = pl.ds(0, 4 - (1 if part == 1 else 0))
        return to_z(
            1, 0, zsend.at[q, part, few], zrecv.at[q, part, few], zs.at[q, part], zr.at[q, part]
        )

    def all_sums(q):
        few = pl.ds(0, 15)
        return to_z(1, 0, crecv.at[q, few], crecv.at[q, few], cs.at[q], cr.at[q])

    def after_y(q, part):
        for p, r in y_peers(q):
            y_copy(q, part, p, r).wait_recv()
        own, got = y_refs(q, part)
        if part == 0:
            csend[q] = own[0, 0, 64:65] + sum(got[p, r, 64:65] for p, r in y_peers(q))
            crecv[q, 15] = csend[q]
            for i, step in enumerate(Z_STEPS):
                for k in range(2):
                    if step or k:
                        at = i * 2 + k - (1 if i * 2 + k > 6 else 0)
                        to_z(step, k, csend.at[q], crecv.at[q, at], cs.at[q], cr.at[q]).start()
        mine, theirs = own[0, 0, 0:64], got[0, 1, 0:64]
        if q not in DIRECT:
            mine, theirs = mine + got[1, 0, 0:64], theirs + got[1, 1, 0:64]
        zsend[q, part, :, 0] = mine.reshape(4, 16, 128)
        zsend[q, part, :, 1] = theirs.reshape(4, 16, 128)
        for i in range(2):
            step = Z_STEPS[part * 2 + i]
            for k in range(2):
                at = i * 2 + k
                if step or k:
                    to_z(
                        step,
                        k,
                        zsend.at[q, part, at],
                        zrecv.at[q, part, at],
                        zs.at[q, part],
                        zr.at[q, part],
                    ).start()
                else:
                    zrecv[q, part, at] = zsend[q, part, at]

    weighted, row_sum, col_sum = [], [], []

    def after_z(q):
        all_sums(q).wait_recv()
        arriving = jnp.sum(crecv[q], axis=0)
        scale = jnp.log(arriving * (2.0**-14))
        for part in range(NP):
            all_rows(q, part).wait_recv()
        high, low = split(zrecv[q].reshape(512, 128))
        out = dot_nn(unpack_rows[...], high) + dot_nn(unpack_rows[...], low)
        merged[:, q * 128 : (q + 1) * 128] = out
        weighted.append(out * (jnp.log(out * 0.25) - scale))
        row_sum.append(out)
        col_sum.append(arriving)

    def go(step):
        kind, q = step[0], int(step[1])
        if kind == "p":
            pack(q)
        elif kind == "x":
            (after_d if q in DIRECT else after_x)(q)
        elif kind == "z":
            after_z(q)
        else:
            after_y(q, "abcd".index(kind))

    for step in ORDER:
        if step == "tags":
            row_tags()
        elif step == "tokens":
            for i in range(4):
                take_token(i)
                if i < 3:
                    pass_token(i + 1)
        else:
            go(step)

    tsend[0:1] = jnp.sum(sum(weighted).T, axis=0, keepdims=True)
    tsend[1:2] = jnp.sum(sum(row_sum).T, axis=0, keepdims=True)
    tsend[2:3] = sum(col_sum)
    tsend[3:8] = jnp.zeros((5, 128), F32)
    trecv[0] = tsend[...]

    def t_copy(t):
        return pltpu.make_async_remote_copy(
            src_ref=tsend,
            dst_ref=trecv.at[t],
            send_sem=ts,
            recv_sem=tr.at[t],
            device_id=(b, lax.rem(c + t, 8)),
            device_id_type=MESH,
        )

    all_told = pltpu.make_async_remote_copy(
        src_ref=trecv.at[pl.ds(0, 7)],
        dst_ref=trecv.at[pl.ds(0, 7)],
        send_sem=ts,
        recv_sem=tr.at[0],
        device_id=(b, lax.rem(c + 1, 8)),
        device_id_type=MESH,
    )
    for t in range(1, 8):
        t_copy(t).start()
    for q in range(NQ):
        for dx in range(4):
            if q in RELAYED:
                if dx:
                    x_copy(RELAYED.index(q), dx).wait_send()
            else:
                for p in range(2):
                    if p or dx:
                        d_copy(DIRECT.index(q), p, dx).wait_send()
        for part in range(NP):
            for p, r in y_peers(q):
                y_copy(q, part, p, r).wait_send()
            all_rows(q, part).wait_send()
        all_sums(q).wait_send()
    for t in range(1, 8):
        t_copy(t).wait_recv()
    all_told.wait_send()
    everyone = jnp.sum(trecv[...], axis=0)
    out_total = everyone[1:2]
    total = jnp.sum(everyone[2:3], axis=1, keepdims=True)
    terms[...] = (
        everyone[0:1] / out_total
        + jnp.log(total * (2.0**-26))
        - jnp.log(out_total * (2.0**-14))
    )


def shards(counts, merge_map):
    ids = merge_map.reshape(32, 1, 256)
    dma = pltpu.SemaphoreType.DMA
    merged, terms = pl.pallas_call(
        kernel,
        out_shape=(
            jax.ShapeDtypeStruct((128, 512), F32),
            jax.ShapeDtypeStruct((1, 128), F32),
        ),
        in_specs=[
            pl.BlockSpec(memory_space=pltpu.HBM),
            pl.BlockSpec(memory_space=pltpu.HBM),
        ],
        out_specs=(
            pl.BlockSpec(memory_space=pltpu.VMEM),
            pl.BlockSpec(memory_space=pltpu.VMEM),
        ),
        scratch_shapes=[
            pltpu.VMEM((256, 1024), F32),
            pltpu.VMEM((32, 1, 256), I32),
            pltpu.VMEM((2, 256, 1024), BF16),
            pltpu.VMEM((32, 1, 256), I32),
            pltpu.VMEM((max(ND, 1), 2, 4, 2, 4, 16, 1), F32),
            pltpu.VMEM((max(NR, 1), 4, 2, 4, 16, 1), F32),
            pltpu.VMEM((32, 16, 1), F32),
            pltpu.VMEM((128, 512), BF16),
            pltpu.VMEM((512, 256), BF16),
            pltpu.VMEM((max(ND, 1), 2, 4, 128, 128), F32),
            pltpu.VMEM((max(ND, 1), 2, 4, 128, 128), F32),
            pltpu.VMEM((max(NR, 1), 4, 256, 128), F32),
            pltpu.VMEM((max(NR, 1), 4, 256, 128), F32),
            pltpu.VMEM((NQ, 2, 2, 72, 128), F32),
            pltpu.VMEM((NQ, 2, 2, 72, 128), F32),
            pltpu.VMEM((NQ, NP - 1, 2, 2, 64, 128), F32),
            pltpu.VMEM((NQ, NP - 1, 2, 2, 64, 128), F32),
            pltpu.VMEM((NQ, NP, 4, 2, 16, 128), F32),
            pltpu.VMEM((NQ, NP, 4, 2, 16, 128), F32),
            pltpu.VMEM((NQ, 1, 128), F32),
            pltpu.VMEM((NQ, 16, 1, 128), F32),
            pltpu.VMEM((8, 128), F32),
            pltpu.VMEM((8, 8, 128), F32),
            dma,
            dma,
            dma((max(ND, 1), 2, 4)),
            dma((max(ND, 1), 2, 4)),
            dma((max(NR, 1), 4)),
            dma((max(NR, 1), 4)),
            dma((NQ, NP, 2, 2)),
            dma((NQ, NP, 2, 2)),
            dma((NQ, NP)),
            dma((NQ, NP)),
            dma((NQ,)),
            dma((NQ,)),
            dma,
            dma((8,)),
            pltpu.SemaphoreType.REGULAR((4, 2)),
        ],
        compiler_params=pltpu.CompilerParams(
            collective_id=0, has_side_effects=True, vmem_limit_bytes=56_000_000
        ),
    )(counts, ids)
    return merged, terms.reshape(128)


def solution(mesh):
    return jax.shard_map(
        shards,
        mesh=mesh,
        in_specs=(P("blk", "col"), P()),
        out_specs=(P("blk", "col"), P("blk")),
        check_vma=False,
    )
```

```python
import jax
import jax.numpy as jnp
from jax import lax
from jax.experimental import pallas as pl
from jax.experimental.pallas import tpu as pltpu
from jax.sharding import PartitionSpec as P

MESH = pl.DeviceIdType.MESH
F32 = jnp.float32
BF16 = jnp.bfloat16
I32 = jnp.int32
NQ = 4
NP = 4
Z_STEPS = (4, 3, 5, 0, 2, 6, 1, 7)
ORDER = (
    "tokens",
    "p2",
    "x0",
    "p3",
    "tags",
    "a0",
    "x1",
    "b0",
    "c0",
    "d0",
    "x2",
    "a1",
    "b1",
    "c1",
    "d1",
    "z0",
    "x3",
    "a2",
    "b2",
    "c2",
    "d2",
    "z1",
    "a3",
    "b3",
    "c3",
    "d3",
    "z2",
    "z3",
)


def split(v):
    high = v.astype(BF16)
    return high, (v - high.astype(F32)).astype(BF16)


def dot_nn(a, b):
    return lax.dot_general(a, b, (((1,), (0,)), ((), ())), preferred_element_type=F32)


def dot_nt(a, b):
    return lax.dot_general(a, b, (((1,), (1,)), ((), ())), preferred_element_type=F32)


def iota(shape, dim):
    return lax.broadcasted_iota(I32, shape, dim)


def one_hot(mask):
    return jnp.where(mask, 1.0, 0.0).astype(BF16)


def slot_keys(rows):
    owners = [lax.shift_right_logical(r, 7) for r in rows]
    hits = [o == iota((32, 256), 0) for o in owners]
    table = jnp.concatenate([jnp.where(h, 1.0, 0.0) for h in hits], axis=0)
    before = one_hot(iota((256, 256), 0) < iota((256, 256), 1))
    counted = dot_nn(table.astype(BF16), before) * table
    ranks = [
        jnp.sum(counted[i * 32 : (i + 1) * 32], axis=0, keepdims=True).astype(I32)
        for i in range(len(rows))
    ]
    return [o * 16 + r for o, r in zip(owners, ranks)]


def kernel(
    counts_hbm,
    ids_hbm,
    merged,
    terms,
    counts,
    ids,
    parts,
    keys,
    coltag,
    rowtag,
    unpack_rows,
    pack_rows,
    xsend,
    xrecv,
    asend,
    arecv,
    bsend,
    brecv,
    zsend,
    zrecv,
    csend,
    crecv,
    tsend,
    trecv,
    in_sem,
    ids_sem,
    xs,
    xr,
    ys,
    yr,
    zs,
    zr,
    cs,
    cr,
    ts,
    tr,
    token,
):
    b = lax.axis_index("blk")
    c = lax.axis_index("col")
    x, yh = lax.rem(c, 4), lax.div(c, 4)
    core, zz, yl = lax.rem(b, 2), lax.rem(lax.div(b, 2), 8), lax.div(b, 16)

    ids_load = pltpu.make_async_copy(ids_hbm, ids, ids_sem)
    ids_load.start()
    load = pltpu.make_async_copy(counts_hbm, counts, in_sem)
    load.start()

    barrier = pltpu.get_barrier_semaphore()

    def z_peer(step, k):
        return (yl * 8 + lax.rem(zz + step, 8)) * 2 + lax.rem(core + k, 2)

    def y_peer(p, r):
        return lax.rem(yl + r, 2) * 16 + zz * 2 + core, lax.rem(c + 4 * p, 8)

    def greet(peer):
        pl.semaphore_signal(barrier, inc=1, device_id=peer, device_id_type=MESH)

    for dx in range(1, 4):
        greet((b, yh * 4 + lax.rem(x + dx, 4)))
    for p, r in ((1, 0), (0, 1), (1, 1)):
        greet(y_peer(p, r))
    for step, k in ((1, 0), (7, 0), (0, 1)):
        greet((z_peer(step, k), c))

    ids_load.wait()
    positions = []
    for g, key in enumerate(slot_keys([ids[c * 4 + g] for g in range(4)])):
        owner = lax.shift_right_logical(key, 4)
        to = lax.shift_right_logical(owner, 2)
        dx = (to - x) & 3
        tile = jnp.where(dx == 2, 0, jnp.where(dx == 1, 1, jnp.where(dx == 3, 2, 3)))
        half = (lax.shift_right_logical(to, 2) - yh) & 1
        positions.append((owner & 3) * 512 + tile * 128 + half * 64 + g * 16 + (key & 15))
    position = jnp.concatenate(positions, axis=1)

    load.wait()
    high, low = split(counts[...])
    parts[0] = high
    parts[1] = low

    def x_copy(q, dx):
        return pltpu.make_async_remote_copy(
            src_ref=xsend.at[q, dx],
            dst_ref=xrecv.at[q, dx],
            send_sem=xs,
            recv_sem=xr.at[q],
            device_id=(b, yh * 4 + lax.rem(x + dx, 4)),
            device_id_type=MESH,
        )

    def all_columns(refs, recv):
        return pltpu.make_async_remote_copy(
            src_ref=refs,
            dst_ref=refs,
            send_sem=xs,
            recv_sem=recv,
            device_id=(b, yh * 4 + lax.rem(x + 1, 4)),
            device_id_type=MESH,
        )

    def pack(q):
        for first, tiles in ((0, (2, 1)), (256, (3, 0))):
            pick = one_hot(position - q * 512 == iota((256, 1024), 0) + first)
            packed = dot_nt(parts[0], pick) + dot_nt(parts[1], pick)
            for i, dx in enumerate(tiles):
                value = packed[:, i * 128 : (i + 1) * 128]
                if dx == 0:
                    xrecv[q, 0] = value
                else:
                    xsend[q, dx] = value
                    if q > 0:
                        x_copy(q, dx).start()

    sixteen = iota((16, 1), 0)

    def pass_token():
        for way, step in enumerate((1, 7)):
            pl.semaphore_signal(
                token.at[way], inc=1, device_id=(z_peer(step, 0), c), device_id_type=MESH
            )

    def take_token():
        for way in range(2):
            pl.semaphore_wait(token.at[way], 1)


    def all_keys():
        for i in range(4):
            for g, key in enumerate(slot_keys([ids[i * 8 + g] for g in range(8)])):
                keys[i * 8 + g] = key

    def column_tags():
        owners = [(lax.rem(yh + p, 2) * 4 + x) * 4 + q for q in range(NQ) for p in range(2)]
        wanted = jnp.concatenate([o * 16 + sixteen for o in owners], axis=0)
        for dx in range(4):
            for g in range(4):
                src = yh * 16 + lax.rem(x + 4 - dx, 4) * 4 + g
                value = ((ids[src] & 127) + 1).astype(F32)
                tag = jnp.sum(jnp.where(keys[src] == wanted, value, 0.0), axis=1, keepdims=True)
                other = jnp.where(tag > 0.0, tag + 128.0, 0.0)
                for q in range(NQ):
                    coltag[q, dx, 0, g] = tag[q * 32 : q * 32 + 16]
                    coltag[q, dx, 1, g] = other[q * 32 + 16 : q * 32 + 32]

    def row_places():
        key = keys[b]
        owner = lax.shift_right_logical(key, 4)
        k = (owner - core) & 1
        dz = (lax.shift_right_logical(owner, 1) - zz) & 7
        r = (lax.shift_right_logical(owner, 4) - yl) & 1
        at = sum(jnp.where(dz == step, i, 0) for i, step in enumerate(Z_STEPS))
        place = (at >> 1) * 128 + r * 64 + (at & 1) * 32 + k * 16 + (key & 15)
        pack_rows[...] = one_hot(place == iota((512, 256), 0))

    def row_tags():
        for i, step in enumerate(Z_STEPS):
            for k in range(2):
                for r in range(2):
                    z = lax.rem(zz + 8 - step, 8)
                    src = (lax.rem(yl + r, 2) * 8 + z) * 2 + lax.rem(core + k, 2)
                    value = ((ids[src] & 127) + 1).astype(F32)
                    hit = keys[src] == b * 16 + sixteen
                    rowtag[(i * 2 + k) * 2 + r] = jnp.sum(
                        jnp.where(hit, value, 0.0), axis=1, keepdims=True
                    )
        flat = rowtag[...].reshape(512, 1).astype(I32)
        unpack_rows[...] = jnp.where(flat == iota((512, 128), 1) + 1, 1.0, 0.0).T.astype(BF16)

    pack(0)
    pl.semaphore_wait(barrier, 9)
    for dx in (2, 1, 3):
        x_copy(0, dx).start()
    pass_token()
    pack(1)
    all_keys()
    column_tags()
    row_places()

    Y_PEERS = ((1, 0), (1, 1), (0, 1))

    def y_refs(q, part):
        if part == 0:
            return asend.at[q], arecv.at[q]
        return bsend.at[q, part - 1], brecv.at[q, part - 1]

    def y_copy(q, part, p, r, few=False):
        src, dst = y_refs(q, part)
        at = pl.ds(0, 3) if few else p * 2 + r
        return pltpu.make_async_remote_copy(
            src_ref=src.at[at],
            dst_ref=dst.at[at],
            send_sem=ys.at[min(part, 1)],
            recv_sem=yr.at[q, part],
            device_id=y_peer(p, r),
            device_id_type=MESH,
        )

    def after_x(q):
        tag = coltag[q].reshape(512, 1).astype(I32)
        place = one_hot(tag == iota((512, 256), 1) + 1)
        all_columns(xrecv.at[q, pl.ds(0, 3)], xr.at[q]).wait_recv()
        got = jnp.concatenate([xrecv[q, dx] for dx in range(4)], axis=1)
        high, low = split(got)
        block = dot_nn(high, place) + dot_nn(low, place)
        sums = jnp.sum(block, axis=0, keepdims=True)
        high, low = split(block)
        for part in range(NP):
            pick = pack_rows[part * 128 : (part + 1) * 128]
            packed = dot_nn(pick, high) + dot_nn(pick, low)
            out = y_refs(q, part)[0]
            for p in range(2):
                for r in range(2):
                    at = r * 64
                    out[p * 2 + r, 0:64] = packed[at : at + 64, p * 128 : (p + 1) * 128]
                    if part == 0:
                        out[p * 2 + r, 64:72] = jnp.broadcast_to(
                            sums[:, p * 128 : (p + 1) * 128], (8, 128)
                        )
            for p, r in Y_PEERS:
                y_copy(q, part, p, r).start()

    def all_sends(refs, send):
        return pltpu.make_async_remote_copy(
            src_ref=refs,
            dst_ref=refs,
            send_sem=send,
            recv_sem=yr.at[0, 0],
            device_id=y_peer(0, 1),
            device_id_type=MESH,
        )

    def to_z(step, k, src, dst, send, recv):
        return pltpu.make_async_remote_copy(
            src_ref=src,
            dst_ref=dst,
            send_sem=send,
            recv_sem=recv,
            device_id=(z_peer(step, k), c),
            device_id_type=MESH,
        )

    def all_rows(refs, recv):
        return to_z(1, 0, refs, refs, zs, recv)

    def all_sums(refs, recv):
        return to_z(1, 0, refs, refs, cs, recv)

    def after_y(q, part):
        y_copy(q, part, 1, 0, few=True).wait_recv()
        own, got = y_refs(q, part)
        to = (q * NP + part) * 4
        if part == 0:
            csend[q] = own[0, 64:65] + got[1, 64:65] + got[2, 64:65] + got[3, 64:65]
            crecv[q * 16 + 15] = csend[q]
            for i, step in enumerate(Z_STEPS):
                for k in range(2):
                    if step or k:
                        at = q * 16 + i * 2 + k - (1 if i * 2 + k > 6 else 0)
                        to_z(step, k, csend.at[q], crecv.at[at], cs, cr.at[q]).start()
        mine = own[0, 0:64] + got[2, 0:64]
        theirs = got[1, 0:64] + got[3, 0:64]
        zsend[to : to + 4, 0] = mine.reshape(4, 16, 128)
        zsend[to : to + 4, 1] = theirs.reshape(4, 16, 128)
        for i in range(2):
            step = Z_STEPS[part * 2 + i]
            for k in range(2):
                at = to + i * 2 + k
                if step or k:
                    to_z(step, k, zsend.at[at], zrecv.at[at], zs, zr.at[q]).start()
                else:
                    zrecv[at] = zsend[at]

    weighted, row_sum, col_sum = [], [], []

    def after_z(q):
        all_sums(crecv.at[pl.ds(q * 16, 15)], cr.at[q]).wait_recv()
        arriving = jnp.sum(crecv[q * 16 : q * 16 + 16], axis=0)
        scale = jnp.log(arriving * (2.0**-14))
        all_rows(zrecv.at[pl.ds(q * 16, 15)], zr.at[q]).wait_recv()
        high, low = split(zrecv[q * 16 : (q + 1) * 16].reshape(512, 128))
        out = dot_nn(unpack_rows[...], high) + dot_nn(unpack_rows[...], low)
        merged[:, q * 128 : (q + 1) * 128] = out
        weighted.append(out * (jnp.log(out * 0.25) - scale))
        row_sum.append(out)
        col_sum.append(arriving)

    def go(step):
        kind, q = step[0], int(step[1])
        if kind == "p":
            pack(q)
        elif kind == "x":
            after_x(q)
        elif kind == "z":
            after_z(q)
        else:
            after_y(q, "abcd".index(kind))

    for step in ORDER:
        if step == "tags":
            row_tags()
        elif step == "tokens":
            for i in range(4):
                take_token()
                if i < 3:
                    pass_token()
        else:
            go(step)

    tsend[0:1] = jnp.sum(sum(weighted).T, axis=0, keepdims=True)
    tsend[1:2] = jnp.sum(sum(row_sum).T, axis=0, keepdims=True)
    tsend[2:3] = sum(col_sum)
    tsend[3:8] = jnp.zeros((5, 128), F32)
    trecv[0] = tsend[...]

    def t_copy(t):
        return pltpu.make_async_remote_copy(
            src_ref=tsend,
            dst_ref=trecv.at[t],
            send_sem=ts,
            recv_sem=tr,
            device_id=(b, lax.rem(c + t, 8)),
            device_id_type=MESH,
        )

    all_told = pltpu.make_async_remote_copy(
        src_ref=trecv.at[pl.ds(0, 7)],
        dst_ref=trecv.at[pl.ds(0, 7)],
        send_sem=ts,
        recv_sem=tr,
        device_id=(b, lax.rem(c + 1, 8)),
        device_id_type=MESH,
    )
    for t in range(1, 8):
        t_copy(t).start()
    all_columns(xsend.at[pl.ds(0, 3)], xr.at[0]).wait_send()
    all_sends(asend.at[pl.ds(0, 3)], ys.at[0]).wait_send()
    all_sends(bsend.at[pl.ds(0, 3)], ys.at[1]).wait_send()
    all_rows(zsend.at[pl.ds(0, 60)], zr.at[0]).wait_send()
    all_sums(crecv.at[pl.ds(0, 60)], cr.at[0]).wait_send()
    all_told.wait_recv()
    all_told.wait_send()
    everyone = jnp.sum(trecv[...], axis=0)
    out_total = everyone[1:2]
    total = jnp.sum(everyone[2:3], axis=1, keepdims=True)
    terms[...] = (
        everyone[0:1] / out_total
        + jnp.log(total * (2.0**-26))
        - jnp.log(out_total * (2.0**-14))
    )


def shards(counts, merge_map):
    ids = merge_map.reshape(32, 1, 256)
    dma = pltpu.SemaphoreType.DMA
    merged, terms = pl.pallas_call(
        kernel,
        out_shape=(
            jax.ShapeDtypeStruct((128, 512), F32),
            jax.ShapeDtypeStruct((1, 128), F32),
        ),
        in_specs=[
            pl.BlockSpec(memory_space=pltpu.HBM),
            pl.BlockSpec(memory_space=pltpu.HBM),
        ],
        out_specs=(
            pl.BlockSpec(memory_space=pltpu.VMEM),
            pl.BlockSpec(memory_space=pltpu.VMEM),
        ),
        scratch_shapes=[
            pltpu.VMEM((256, 1024), F32),
            pltpu.VMEM((32, 1, 256), I32),
            pltpu.VMEM((2, 256, 1024), BF16),
            pltpu.VMEM((32, 1, 256), I32),
            pltpu.VMEM((NQ, 4, 2, 4, 16, 1), F32),
            pltpu.VMEM((32, 16, 1), F32),
            pltpu.VMEM((128, 512), BF16),
            pltpu.VMEM((512, 256), BF16),
            pltpu.VMEM((NQ, 4, 256, 128), F32),
            pltpu.VMEM((NQ, 4, 256, 128), F32),
            pltpu.VMEM((NQ, 4, 72, 128), F32),
            pltpu.VMEM((NQ, 4, 72, 128), F32),
            pltpu.VMEM((NQ, NP - 1, 4, 64, 128), F32),
            pltpu.VMEM((NQ, NP - 1, 4, 64, 128), F32),
            pltpu.VMEM((NQ * 16, 2, 16, 128), F32),
            pltpu.VMEM((NQ * 16, 2, 16, 128), F32),
            pltpu.VMEM((NQ, 1, 128), F32),
            pltpu.VMEM((NQ * 16, 1, 128), F32),
            pltpu.VMEM((8, 128), F32),
            pltpu.VMEM((8, 8, 128), F32),
            dma,
            dma,
            dma,
            dma((NQ,)),
            dma((2,)),
            dma((NQ, NP)),
            dma,
            dma((NQ,)),
            dma,
            dma((NQ,)),
            dma,
            dma,
            pltpu.SemaphoreType.REGULAR((2,)),
        ],
        compiler_params=pltpu.CompilerParams(
            collective_id=0, has_side_effects=True, vmem_limit_bytes=56_000_000
        ),
    )(counts, ids)
    return merged, terms.reshape(128)


def solution(mesh):
    return jax.shard_map(
        shards,
        mesh=mesh,
        in_specs=(P("blk", "col"), P()),
        out_specs=(P("blk", "col"), P("blk")),
        check_vma=False,
    )
```

```python
import jax
import jax.numpy as jnp
from jax import lax
from jax.experimental import pallas as pl
from jax.experimental.pallas import tpu as pltpu
from jax.sharding import PartitionSpec as P

MESH = pl.DeviceIdType.MESH
F32 = jnp.float32
BF16 = jnp.bfloat16
I32 = jnp.int32
NQ = 4
NP = 4
Z_STEPS = (3, 5, 4, 0, 2, 6, 1, 7)
OWN = 2 * Z_STEPS.index(0)
ORDER = (
    "p2",
    "tokens",
    "x0",
    "p3",
    "tags",
    "a0",
    "x1",
    "b0",
    "c0",
    "d0",
    "a1",
    "x2",
    "b1",
    "c1",
    "d1",
    "z0",
    "x3",
    "a2",
    "b2",
    "c2",
    "d2",
    "z1",
    "a3",
    "b3",
    "c3",
    "d3",
    "z2",
    "z3",
)


def split(v):
    high = v.astype(BF16)
    return high, (v - high.astype(F32)).astype(BF16)


def dot_nn(a, b):
    return lax.dot_general(a, b, (((1,), (0,)), ((), ())), preferred_element_type=F32)


def dot_nt(a, b):
    return lax.dot_general(a, b, (((1,), (1,)), ((), ())), preferred_element_type=F32)


def iota(shape, dim):
    return lax.broadcasted_iota(I32, shape, dim)


def one_hot(mask):
    return jnp.where(mask, 1.0, 0.0).astype(BF16)


def slot_keys(rows):
    owners = [lax.shift_right_logical(r, 7) for r in rows]
    hits = [o == iota((32, 256), 0) for o in owners]
    table = jnp.concatenate([jnp.where(h, 1.0, 0.0) for h in hits], axis=0)
    before = one_hot(iota((256, 256), 0) < iota((256, 256), 1))
    counted = dot_nn(table.astype(BF16), before) * table
    ranks = [
        jnp.sum(counted[i * 32 : (i + 1) * 32], axis=0, keepdims=True).astype(I32)
        for i in range(len(rows))
    ]
    return [o * 16 + r for o, r in zip(owners, ranks)]


def kernel(
    counts_hbm,
    ids,
    merged,
    terms,
    counts,
    parts,
    keys,
    coltag,
    rowtag,
    unpack_rows,
    pack_rows,
    xsend,
    xrecv,
    asend,
    arecv,
    bsend,
    brecv,
    zsend,
    zrecv,
    csend,
    crecv,
    tsend,
    trecv,
    in_sem,
    xs,
    xr,
    ys,
    yr,
    zs,
    zr,
    cs,
    cr,
    ts,
    tr,
    token,
):
    b = lax.axis_index("blk")
    c = lax.axis_index("col")
    x, yh = lax.rem(c, 4), lax.div(c, 4)
    core, zz, yl = lax.rem(b, 2), lax.rem(lax.div(b, 2), 8), lax.div(b, 16)

    load = pltpu.make_async_copy(counts_hbm, counts, in_sem)
    load.start()

    barrier = pltpu.get_barrier_semaphore()

    def z_peer(step, k):
        return (yl * 8 + lax.rem(zz + step, 8)) * 2 + lax.rem(core + k, 2)

    def y_peer(p, r):
        return lax.rem(yl + r, 2) * 16 + zz * 2 + core, lax.rem(c + 4 * p, 8)

    def greet(peer):
        pl.semaphore_signal(barrier, inc=1, device_id=peer, device_id_type=MESH)

    for dx in range(1, 4):
        greet((b, yh * 4 + lax.rem(x + dx, 4)))
    for p, r in ((1, 0), (0, 1), (1, 1)):
        greet(y_peer(p, r))
    for step, k in ((1, 0), (7, 0), (0, 1)):
        greet((z_peer(step, k), c))

    positions = []
    for g, key in enumerate(slot_keys([ids[c * 4 + g] for g in range(4)])):
        owner = lax.shift_right_logical(key, 4)
        to = lax.shift_right_logical(owner, 2)
        dx = (to - x) & 3
        tile = jnp.where(dx == 2, 0, jnp.where(dx == 1, 1, jnp.where(dx == 3, 2, 3)))
        half = (lax.shift_right_logical(to, 2) - yh) & 1
        positions.append((owner & 3) * 512 + tile * 128 + half * 64 + g * 16 + (key & 15))
    position = jnp.concatenate(positions, axis=1)

    load.wait()
    high, low = split(counts[...])
    parts[0] = high
    parts[1] = low

    def x_copy(q, dx):
        return pltpu.make_async_remote_copy(
            src_ref=xsend.at[q, dx],
            dst_ref=xrecv.at[q, dx],
            send_sem=xs,
            recv_sem=xr.at[q],
            device_id=(b, yh * 4 + lax.rem(x + dx, 4)),
            device_id_type=MESH,
        )

    def all_columns(refs, recv):
        return pltpu.make_async_remote_copy(
            src_ref=refs,
            dst_ref=refs,
            send_sem=xs,
            recv_sem=recv,
            device_id=(b, yh * 4 + lax.rem(x + 1, 4)),
            device_id_type=MESH,
        )

    def pack(q):
        for first, tiles in ((0, (2, 1)), (256, (3, 0))):
            pick = one_hot(position - q * 512 == iota((256, 1024), 0) + first)
            packed = dot_nt(parts[0], pick) + dot_nt(parts[1], pick)
            for i, dx in enumerate(tiles):
                value = packed[:, i * 128 : (i + 1) * 128]
                if dx == 0:
                    xrecv[q, 0] = value
                else:
                    xsend[q, dx] = value
                    if q > 0:
                        x_copy(q, dx).start()

    sixteen = iota((16, 1), 0)

    def pass_token():
        for way, step in enumerate((1, 7)):
            pl.semaphore_signal(
                token.at[way], inc=1, device_id=(z_peer(step, 0), c), device_id_type=MESH
            )

    def take_token():
        for way in range(2):
            pl.semaphore_wait(token.at[way], 1)


    def all_keys():
        for i in range(4):
            for g, key in enumerate(slot_keys([ids[i * 8 + g] for g in range(8)])):
                keys[i * 8 + g] = key

    def column_tags():
        owners = [(lax.rem(yh + p, 2) * 4 + x) * 4 + q for q in range(NQ) for p in range(2)]
        wanted = jnp.concatenate([o * 16 + sixteen for o in owners], axis=0)
        for dx in range(4):
            for g in range(4):
                src = yh * 16 + lax.rem(x + 4 - dx, 4) * 4 + g
                value = ((ids[src] & 127) + 1).astype(F32)
                tag = jnp.sum(jnp.where(keys[src] == wanted, value, 0.0), axis=1, keepdims=True)
                other = jnp.where(tag > 0.0, tag + 128.0, 0.0)
                for q in range(NQ):
                    coltag[q, dx, 0, g] = tag[q * 32 : q * 32 + 16]
                    coltag[q, dx, 1, g] = other[q * 32 + 16 : q * 32 + 32]

    def row_places():
        key = keys[b]
        owner = lax.shift_right_logical(key, 4)
        k = (owner - core) & 1
        dz = (lax.shift_right_logical(owner, 1) - zz) & 7
        r = (lax.shift_right_logical(owner, 4) - yl) & 1
        at = sum(jnp.where(dz == step, i, 0) for i, step in enumerate(Z_STEPS))
        place = (at >> 1) * 128 + r * 64 + (at & 1) * 32 + k * 16 + (key & 15)
        pack_rows[...] = one_hot(place == iota((512, 256), 0))

    def row_tags():
        for i, step in enumerate(Z_STEPS):
            for k in range(2):
                for r in range(2):
                    z = lax.rem(zz + 8 - step, 8)
                    src = (lax.rem(yl + r, 2) * 8 + z) * 2 + lax.rem(core + k, 2)
                    value = ((ids[src] & 127) + 1).astype(F32)
                    hit = keys[src] == b * 16 + sixteen
                    rowtag[(i * 2 + k) * 2 + r] = jnp.sum(
                        jnp.where(hit, value, 0.0), axis=1, keepdims=True
                    )
        flat = rowtag[...].reshape(512, 1).astype(I32)
        unpack_rows[...] = jnp.where(flat == iota((512, 128), 1) + 1, 1.0, 0.0).T.astype(BF16)

    pack(0)
    pl.semaphore_wait(barrier, 9)
    for dx in (2, 1, 3):
        x_copy(0, dx).start()
    pass_token()
    pack(1)
    all_keys()
    column_tags()
    row_places()

    Y_PEERS = ((1, 0), (1, 1), (0, 1))

    def y_refs(q, part):
        if part == 0:
            return asend.at[q], arecv.at[q]
        return bsend.at[q, part - 1], brecv.at[q, part - 1]

    def y_copy(q, part, p, r, few=False):
        src, dst = y_refs(q, part)
        at = pl.ds(0, 3) if few else p * 2 + r
        return pltpu.make_async_remote_copy(
            src_ref=src.at[at],
            dst_ref=dst.at[at],
            send_sem=ys.at[min(part, 1)],
            recv_sem=yr.at[q, part],
            device_id=y_peer(p, r),
            device_id_type=MESH,
        )

    def after_x(q):
        tag = coltag[q].reshape(512, 1).astype(I32)
        place = one_hot(tag == iota((512, 256), 1) + 1)
        all_columns(xrecv.at[q, pl.ds(0, 3)], xr.at[q]).wait_recv()
        got = jnp.concatenate([xrecv[q, dx] for dx in range(4)], axis=1)
        high, low = split(got)
        block = dot_nn(high, place) + dot_nn(low, place)
        sums = jnp.sum(block, axis=0, keepdims=True)
        high, low = split(block)
        for part in range(NP):
            pick = pack_rows[part * 128 : (part + 1) * 128]
            packed = dot_nn(pick, high) + dot_nn(pick, low)
            out = y_refs(q, part)[0]
            for p in range(2):
                for r in range(2):
                    at = r * 64
                    out[p * 2 + r, 0:64] = packed[at : at + 64, p * 128 : (p + 1) * 128]
                    if part == 0:
                        out[p * 2 + r, 64:72] = jnp.broadcast_to(
                            sums[:, p * 128 : (p + 1) * 128], (8, 128)
                        )
            for p, r in Y_PEERS:
                y_copy(q, part, p, r).start()

    def all_sends(refs, send):
        return pltpu.make_async_remote_copy(
            src_ref=refs,
            dst_ref=refs,
            send_sem=send,
            recv_sem=yr.at[0, 0],
            device_id=y_peer(0, 1),
            device_id_type=MESH,
        )

    def to_z(step, k, src, dst, send, recv):
        return pltpu.make_async_remote_copy(
            src_ref=src,
            dst_ref=dst,
            send_sem=send,
            recv_sem=recv,
            device_id=(z_peer(step, k), c),
            device_id_type=MESH,
        )

    def all_rows(refs, recv):
        return to_z(1, 0, refs, refs, zs, recv)

    def all_sums(refs, recv):
        return to_z(1, 0, refs, refs, cs, recv)

    def after_y(q, part):
        y_copy(q, part, 1, 0, few=True).wait_recv()
        own, got = y_refs(q, part)
        to = (q * NP + part) * 4
        if part == 0:
            csend[q] = own[0, 64:65] + got[1, 64:65] + got[2, 64:65] + got[3, 64:65]
            crecv[q * 16 + 15] = csend[q]
            for i, step in enumerate(Z_STEPS):
                for k in range(2):
                    if step or k:
                        at = q * 16 + i * 2 + k - (1 if i * 2 + k > OWN else 0)
                        to_z(step, k, csend.at[q], crecv.at[at], cs, cr.at[q]).start()
        mine = own[0, 0:64] + got[2, 0:64]
        theirs = got[1, 0:64] + got[3, 0:64]
        zsend[to : to + 4, 0] = mine.reshape(4, 16, 128)
        zsend[to : to + 4, 1] = theirs.reshape(4, 16, 128)
        for i in range(2):
            step = Z_STEPS[part * 2 + i]
            for k in range(2):
                at = to + i * 2 + k
                if step or k:
                    to_z(step, k, zsend.at[at], zrecv.at[at], zs, zr.at[q]).start()
                else:
                    zrecv[at] = zsend[at]

    weighted, row_sum, col_sum = [], [], []

    def after_z(q):
        all_sums(crecv.at[pl.ds(q * 16, 15)], cr.at[q]).wait_recv()
        arriving = jnp.sum(crecv[q * 16 : q * 16 + 16], axis=0)
        scale = jnp.log(arriving * (2.0**-14))
        all_rows(zrecv.at[pl.ds(q * 16, 15)], zr.at[q]).wait_recv()
        high, low = split(zrecv[q * 16 : (q + 1) * 16].reshape(512, 128))
        out = dot_nn(unpack_rows[...], high) + dot_nn(unpack_rows[...], low)
        merged[:, q * 128 : (q + 1) * 128] = out
        weighted.append(out * (jnp.log(out * 0.25) - scale))
        row_sum.append(out)
        col_sum.append(arriving)

    def go(step):
        kind, q = step[0], int(step[1])
        if kind == "p":
            pack(q)
        elif kind == "x":
            after_x(q)
        elif kind == "z":
            after_z(q)
        else:
            after_y(q, "abcd".index(kind))

    for step in ORDER:
        if step == "tags":
            row_tags()
        elif step == "tokens":
            for i in range(4):
                take_token()
                if i < 3:
                    pass_token()
        else:
            go(step)

    tsend[0:1] = jnp.sum(sum(weighted).T, axis=0, keepdims=True)
    tsend[1:2] = jnp.sum(sum(row_sum).T, axis=0, keepdims=True)
    tsend[2:3] = sum(col_sum)
    tsend[3:8] = jnp.zeros((5, 128), F32)
    trecv[0] = tsend[...]

    def t_copy(t):
        return pltpu.make_async_remote_copy(
            src_ref=tsend,
            dst_ref=trecv.at[t],
            send_sem=ts,
            recv_sem=tr,
            device_id=(b, lax.rem(c + t, 8)),
            device_id_type=MESH,
        )

    all_told = pltpu.make_async_remote_copy(
        src_ref=trecv.at[pl.ds(0, 7)],
        dst_ref=trecv.at[pl.ds(0, 7)],
        send_sem=ts,
        recv_sem=tr,
        device_id=(b, lax.rem(c + 1, 8)),
        device_id_type=MESH,
    )
    for t in range(1, 8):
        t_copy(t).start()
    all_columns(xsend.at[pl.ds(0, 3)], xr.at[0]).wait_send()
    all_sends(asend.at[pl.ds(0, 3)], ys.at[0]).wait_send()
    all_sends(bsend.at[pl.ds(0, 3)], ys.at[1]).wait_send()
    all_rows(zsend.at[pl.ds(0, 60)], zr.at[0]).wait_send()
    all_sums(crecv.at[pl.ds(0, 60)], cr.at[0]).wait_send()
    all_told.wait_recv()
    all_told.wait_send()
    everyone = jnp.sum(trecv[...], axis=0)
    out_total = everyone[1:2]
    total = jnp.sum(everyone[2:3], axis=1, keepdims=True)
    terms[...] = (
        everyone[0:1] / out_total
        + jnp.log(total * (2.0**-26))
        - jnp.log(out_total * (2.0**-14))
    )


def shards(counts, merge_map):
    ids = merge_map.reshape(32, 1, 256)
    dma = pltpu.SemaphoreType.DMA
    merged, terms = pl.pallas_call(
        kernel,
        out_shape=(
            jax.ShapeDtypeStruct((128, 512), F32),
            jax.ShapeDtypeStruct((1, 128), F32),
        ),
        in_specs=[
            pl.BlockSpec(memory_space=pltpu.HBM),
            pl.BlockSpec(memory_space=pltpu.VMEM),
        ],
        out_specs=(
            pl.BlockSpec(memory_space=pltpu.VMEM),
            pl.BlockSpec(memory_space=pltpu.VMEM),
        ),
        scratch_shapes=[
            pltpu.VMEM((256, 1024), F32),
            pltpu.VMEM((2, 256, 1024), BF16),
            pltpu.VMEM((32, 1, 256), I32),
            pltpu.VMEM((NQ, 4, 2, 4, 16, 1), F32),
            pltpu.VMEM((32, 16, 1), F32),
            pltpu.VMEM((128, 512), BF16),
            pltpu.VMEM((512, 256), BF16),
            pltpu.VMEM((NQ, 4, 256, 128), F32),
            pltpu.VMEM((NQ, 4, 256, 128), F32),
            pltpu.VMEM((NQ, 4, 72, 128), F32),
            pltpu.VMEM((NQ, 4, 72, 128), F32),
            pltpu.VMEM((NQ, NP - 1, 4, 64, 128), F32),
            pltpu.VMEM((NQ, NP - 1, 4, 64, 128), F32),
            pltpu.VMEM((NQ * 16, 2, 16, 128), F32),
            pltpu.VMEM((NQ * 16, 2, 16, 128), F32),
            pltpu.VMEM((NQ, 1, 128), F32),
            pltpu.VMEM((NQ * 16, 1, 128), F32),
            pltpu.VMEM((8, 128), F32),
            pltpu.VMEM((8, 8, 128), F32),
            dma,
            dma,
            dma((NQ,)),
            dma((2,)),
            dma((NQ, NP)),
            dma,
            dma((NQ,)),
            dma,
            dma((NQ,)),
            dma,
            dma,
            pltpu.SemaphoreType.REGULAR((2,)),
        ],
        compiler_params=pltpu.CompilerParams(
            collective_id=0, has_side_effects=True, vmem_limit_bytes=56_000_000
        ),
    )(counts, ids)
    return merged, terms.reshape(128)


def solution(mesh):
    return jax.shard_map(
        shards,
        mesh=mesh,
        in_specs=(P("blk", "col"), P()),
        out_specs=(P("blk", "col"), P("blk")),
        check_vma=False,
    )
```

```python
import jax
import jax.numpy as jnp
from jax import lax
from jax.experimental import pallas as pl
from jax.experimental.pallas import tpu as pltpu
from jax.sharding import PartitionSpec as P

MESH = pl.DeviceIdType.MESH
F32 = jnp.float32
BF16 = jnp.bfloat16
I32 = jnp.int32
NQ = 4
NP = 4
Z_STEPS = (3, 5, 4, 0, 2, 6, 1, 7)
OWN = 2 * Z_STEPS.index(0)
ORDER = (
    "p2",
    "tokens",
    "x0",
    "p3",
    "tags",
    "a0",
    "x1",
    "b0",
    "c0",
    "d0",
    "a1",
    "x2",
    "b1",
    "c1",
    "d1",
    "z0",
    "x3",
    "a2",
    "b2",
    "c2",
    "d2",
    "z1",
    "a3",
    "b3",
    "c3",
    "d3",
    "z2",
    "z3",
)


def split(v):
    high = v.astype(BF16)
    return high, (v - high.astype(F32)).astype(BF16)


def dot_nn(a, b):
    return lax.dot_general(a, b, (((1,), (0,)), ((), ())), preferred_element_type=F32)


def dot_nt(a, b):
    return lax.dot_general(a, b, (((1,), (1,)), ((), ())), preferred_element_type=F32)


def iota(shape, dim):
    return lax.broadcasted_iota(I32, shape, dim)


def one_hot(mask):
    return jnp.where(mask, 1.0, 0.0).astype(BF16)


def slot_keys(rows):
    owners = [lax.shift_right_logical(r, 7) for r in rows]
    hits = [o == iota((32, 256), 0) for o in owners]
    table = jnp.concatenate([jnp.where(h, 1.0, 0.0) for h in hits], axis=0)
    before = one_hot(iota((256, 256), 0) < iota((256, 256), 1))
    counted = dot_nn(table.astype(BF16), before) * table
    ranks = [
        jnp.sum(counted[i * 32 : (i + 1) * 32], axis=0, keepdims=True).astype(I32)
        for i in range(len(rows))
    ]
    return [o * 16 + r for o, r in zip(owners, ranks)]


def kernel(
    counts_hbm,
    ids,
    merged,
    terms,
    counts,
    parts,
    keys,
    coltag,
    rowtag,
    unpack_rows,
    pack_rows,
    xsend,
    xrecv,
    asend,
    arecv,
    bsend,
    brecv,
    zsend,
    zrecv,
    csend,
    crecv,
    tsend,
    trecv,
    in_sem,
    xs,
    xr,
    ys,
    yr,
    zs,
    zr,
    cs,
    cr,
    ts,
    tr,
    token,
):
    b = lax.axis_index("blk")
    c = lax.axis_index("col")
    x, yh = lax.rem(c, 4), lax.div(c, 4)
    core, zz, yl = lax.rem(b, 2), lax.rem(lax.div(b, 2), 8), lax.div(b, 16)

    load = pltpu.make_async_copy(counts_hbm, counts, in_sem)
    load.start()

    barrier = pltpu.get_barrier_semaphore()

    def z_peer(step, k):
        return (yl * 8 + lax.rem(zz + step, 8)) * 2 + lax.rem(core + k, 2)

    def y_peer(p, r):
        return lax.rem(yl + r, 2) * 16 + zz * 2 + core, lax.rem(c + 4 * p, 8)

    def greet(peer):
        pl.semaphore_signal(barrier, inc=1, device_id=peer, device_id_type=MESH)

    for dx in range(1, 4):
        greet((b, yh * 4 + lax.rem(x + dx, 4)))
    for p, r in ((1, 0), (0, 1), (1, 1)):
        greet(y_peer(p, r))
    for step, k in ((1, 0), (7, 0), (0, 1)):
        greet((z_peer(step, k), c))

    positions = []
    for g, key in enumerate(slot_keys([ids[c * 4 + g] for g in range(4)])):
        owner = lax.shift_right_logical(key, 4)
        to = lax.shift_right_logical(owner, 2)
        dx = (to - x) & 3
        tile = jnp.where(dx == 2, 0, jnp.where(dx == 1, 1, jnp.where(dx == 3, 2, 3)))
        half = (lax.shift_right_logical(to, 2) - yh) & 1
        positions.append((owner & 3) * 512 + tile * 128 + half * 64 + g * 16 + (key & 15))
    position = jnp.concatenate(positions, axis=1)

    load.wait()
    high, low = split(counts[...])
    parts[0] = high
    parts[1] = low

    def x_copy(q, dx):
        return pltpu.make_async_remote_copy(
            src_ref=xsend.at[q, dx],
            dst_ref=xrecv.at[q, dx],
            send_sem=xs,
            recv_sem=xr.at[q],
            device_id=(b, yh * 4 + lax.rem(x + dx, 4)),
            device_id_type=MESH,
        )

    def all_columns(refs, recv):
        return pltpu.make_async_remote_copy(
            src_ref=refs,
            dst_ref=refs,
            send_sem=xs,
            recv_sem=recv,
            device_id=(b, yh * 4 + lax.rem(x + 1, 4)),
            device_id_type=MESH,
        )

    def pack(q):
        for first, tiles in ((0, (2, 1)), (256, (3, 0))):
            pick = one_hot(position - q * 512 == iota((256, 1024), 0) + first)
            packed = dot_nt(parts[0], pick) + dot_nt(parts[1], pick)
            for i, dx in enumerate(tiles):
                value = packed[:, i * 128 : (i + 1) * 128]
                if dx == 0:
                    xrecv[q, 0] = value
                else:
                    xsend[q, dx] = value
                    if q > 0:
                        x_copy(q, dx).start()

    sixteen = iota((16, 1), 0)

    def pass_token():
        for way, step in enumerate((1, 7)):
            pl.semaphore_signal(
                token.at[way], inc=1, device_id=(z_peer(step, 0), c), device_id_type=MESH
            )

    def take_token():
        for way in range(2):
            pl.semaphore_wait(token.at[way], 1)


    def all_keys():
        for i in range(4):
            for g, key in enumerate(slot_keys([ids[i * 8 + g] for g in range(8)])):
                keys[i * 8 + g] = key

    def column_tags():
        owners = [(lax.rem(yh + p, 2) * 4 + x) * 4 + q for q in range(NQ) for p in range(2)]
        wanted = jnp.concatenate([o * 16 + sixteen for o in owners], axis=0)
        for dx in range(4):
            for g in range(4):
                src = yh * 16 + lax.rem(x + 4 - dx, 4) * 4 + g
                value = ((ids[src] & 127) + 1).astype(F32)
                tag = jnp.sum(jnp.where(keys[src] == wanted, value, 0.0), axis=1, keepdims=True)
                other = jnp.where(tag > 0.0, tag + 128.0, 0.0)
                for q in range(NQ):
                    coltag[q, dx, 0, g] = tag[q * 32 : q * 32 + 16]
                    coltag[q, dx, 1, g] = other[q * 32 + 16 : q * 32 + 32]

    def row_places():
        key = keys[b]
        owner = lax.shift_right_logical(key, 4)
        k = (owner - core) & 1
        dz = (lax.shift_right_logical(owner, 1) - zz) & 7
        r = (lax.shift_right_logical(owner, 4) - yl) & 1
        at = sum(jnp.where(dz == step, i, 0) for i, step in enumerate(Z_STEPS))
        place = (at >> 1) * 128 + r * 64 + (at & 1) * 32 + k * 16 + (key & 15)
        pack_rows[...] = one_hot(place == iota((512, 256), 0))

    def row_tags():
        for i, step in enumerate(Z_STEPS):
            for k in range(2):
                for r in range(2):
                    z = lax.rem(zz + 8 - step, 8)
                    src = (lax.rem(yl + r, 2) * 8 + z) * 2 + lax.rem(core + k, 2)
                    value = ((ids[src] & 127) + 1).astype(F32)
                    hit = keys[src] == b * 16 + sixteen
                    rowtag[(i * 2 + k) * 2 + r] = jnp.sum(
                        jnp.where(hit, value, 0.0), axis=1, keepdims=True
                    )
        flat = rowtag[...].reshape(512, 1).astype(I32)
        unpack_rows[...] = jnp.where(flat == iota((512, 128), 1) + 1, 1.0, 0.0).T.astype(BF16)

    pack(0)
    pl.semaphore_wait(barrier, 9)
    for dx in (2, 1, 3):
        x_copy(0, dx).start()
    pass_token()
    pack(1)
    all_keys()
    column_tags()
    row_places()

    Y_PEERS = ((1, 0), (1, 1), (0, 1))

    def y_refs(q, part):
        if part == 0:
            return asend.at[q], arecv.at[q]
        return bsend.at[q, part - 1], brecv.at[q, part - 1]

    def y_copy(q, part, p, r, few=False):
        src, dst = y_refs(q, part)
        at = pl.ds(0, 3) if few else p * 2 + r
        return pltpu.make_async_remote_copy(
            src_ref=src.at[at],
            dst_ref=dst.at[at],
            send_sem=ys.at[min(part, 1)],
            recv_sem=yr.at[q, part],
            device_id=y_peer(p, r),
            device_id_type=MESH,
        )

    def after_x(q):
        tag = coltag[q].reshape(512, 1).astype(I32)
        place = one_hot(tag == iota((512, 256), 1) + 1)
        all_columns(xrecv.at[q, pl.ds(0, 3)], xr.at[q]).wait_recv()
        got = jnp.concatenate([xrecv[q, dx] for dx in range(4)], axis=1)
        high, low = split(got)
        block = dot_nn(high, place) + dot_nn(low, place)
        sums = jnp.sum(block, axis=0, keepdims=True)
        high, low = split(block)
        for part in range(NP):
            pick = pack_rows[part * 128 : (part + 1) * 128]
            packed = dot_nn(pick, high) + dot_nn(pick, low)
            out = y_refs(q, part)[0]
            for p in range(2):
                for r in range(2):
                    at = r * 64
                    out[p * 2 + r, 0:64] = packed[at : at + 64, p * 128 : (p + 1) * 128]
                    if part == 0:
                        out[p * 2 + r, 64:72] = jnp.broadcast_to(
                            sums[:, p * 128 : (p + 1) * 128], (8, 128)
                        )
            for p, r in Y_PEERS:
                y_copy(q, part, p, r).start()

    def all_sends(refs, send):
        return pltpu.make_async_remote_copy(
            src_ref=refs,
            dst_ref=refs,
            send_sem=send,
            recv_sem=yr.at[0, 0],
            device_id=y_peer(0, 1),
            device_id_type=MESH,
        )

    def to_z(step, k, src, dst, send, recv):
        return pltpu.make_async_remote_copy(
            src_ref=src,
            dst_ref=dst,
            send_sem=send,
            recv_sem=recv,
            device_id=(z_peer(step, k), c),
            device_id_type=MESH,
        )

    def all_rows(refs, recv):
        return to_z(1, 0, refs, refs, zs, recv)

    def all_sums(refs, recv):
        return to_z(1, 0, refs, refs, cs, recv)

    def after_y(q, part):
        y_copy(q, part, 1, 0, few=True).wait_recv()
        own, got = y_refs(q, part)
        to = (q * NP + part) * 4
        mine = own[0, 0:64] + got[2, 0:64]
        theirs = got[1, 0:64] + got[3, 0:64]
        zsend[to : to + 4, 0] = mine.reshape(4, 16, 128)
        zsend[to : to + 4, 1] = theirs.reshape(4, 16, 128)
        for i in range(2):
            step = Z_STEPS[part * 2 + i]
            for k in range(2):
                at = to + i * 2 + k
                if step or k:
                    to_z(step, k, zsend.at[at], zrecv.at[at], zs, zr.at[q]).start()
                else:
                    zrecv[at] = zsend[at]
        if part == 0:
            csend[q] = own[0, 64:65] + got[1, 64:65] + got[2, 64:65] + got[3, 64:65]
            crecv[q * 16 + 15] = csend[q]
            for i, step in enumerate(Z_STEPS):
                for k in range(2):
                    if step or k:
                        at = q * 16 + i * 2 + k - (1 if i * 2 + k > OWN else 0)
                        to_z(step, k, csend.at[q], crecv.at[at], cs, cr.at[q]).start()

    weighted, row_sum, col_sum = [], [], []

    def after_z(q):
        all_sums(crecv.at[pl.ds(q * 16, 15)], cr.at[q]).wait_recv()
        arriving = jnp.sum(crecv[q * 16 : q * 16 + 16], axis=0)
        scale = jnp.log(arriving * (2.0**-14))
        all_rows(zrecv.at[pl.ds(q * 16, 15)], zr.at[q]).wait_recv()
        high, low = split(zrecv[q * 16 : (q + 1) * 16].reshape(512, 128))
        out = dot_nn(unpack_rows[...], high) + dot_nn(unpack_rows[...], low)
        merged[:, q * 128 : (q + 1) * 128] = out
        weighted.append(out * (jnp.log(out * 0.25) - scale))
        row_sum.append(out)
        col_sum.append(arriving)

    def go(step):
        kind, q = step[0], int(step[1])
        if kind == "p":
            pack(q)
        elif kind == "x":
            after_x(q)
        elif kind == "z":
            after_z(q)
        else:
            after_y(q, "abcd".index(kind))

    for step in ORDER:
        if step == "tags":
            row_tags()
        elif step == "tokens":
            for i in range(4):
                take_token()
                if i < 3:
                    pass_token()
        else:
            go(step)

    tsend[0:1] = jnp.sum(sum(weighted).T, axis=0, keepdims=True)
    tsend[1:2] = jnp.sum(sum(row_sum).T, axis=0, keepdims=True)
    tsend[2:3] = sum(col_sum)
    tsend[3:8] = jnp.zeros((5, 128), F32)
    trecv[0] = tsend[...]

    def t_copy(t):
        return pltpu.make_async_remote_copy(
            src_ref=tsend,
            dst_ref=trecv.at[t],
            send_sem=ts,
            recv_sem=tr,
            device_id=(b, lax.rem(c + t, 8)),
            device_id_type=MESH,
        )

    all_told = pltpu.make_async_remote_copy(
        src_ref=trecv.at[pl.ds(0, 7)],
        dst_ref=trecv.at[pl.ds(0, 7)],
        send_sem=ts,
        recv_sem=tr,
        device_id=(b, lax.rem(c + 1, 8)),
        device_id_type=MESH,
    )
    for t in range(1, 8):
        t_copy(t).start()
    all_columns(xsend.at[pl.ds(0, 3)], xr.at[0]).wait_send()
    all_sends(asend.at[pl.ds(0, 3)], ys.at[0]).wait_send()
    all_sends(bsend.at[pl.ds(0, 3)], ys.at[1]).wait_send()
    all_rows(zsend.at[pl.ds(0, 60)], zr.at[0]).wait_send()
    all_sums(crecv.at[pl.ds(0, 60)], cr.at[0]).wait_send()
    all_told.wait_recv()
    all_told.wait_send()
    everyone = jnp.sum(trecv[...], axis=0)
    out_total = everyone[1:2]
    total = jnp.sum(everyone[2:3], axis=1, keepdims=True)
    value = (
        everyone[0:1] / out_total
        + jnp.log(total * (2.0**-26))
        - jnp.log(out_total * (2.0**-14))
    )
    terms[...] = value.reshape(128)


def shards(counts, merge_map):
    ids = merge_map.reshape(32, 1, 256)
    dma = pltpu.SemaphoreType.DMA
    merged, terms = pl.pallas_call(
        kernel,
        out_shape=(
            jax.ShapeDtypeStruct((128, 512), F32),
            jax.ShapeDtypeStruct((128,), F32),
        ),
        in_specs=[
            pl.BlockSpec(memory_space=pltpu.HBM),
            pl.BlockSpec(memory_space=pltpu.VMEM),
        ],
        out_specs=(
            pl.BlockSpec(memory_space=pltpu.VMEM),
            pl.BlockSpec(memory_space=pltpu.VMEM),
        ),
        scratch_shapes=[
            pltpu.VMEM((256, 1024), F32),
            pltpu.VMEM((2, 256, 1024), BF16),
            pltpu.VMEM((32, 1, 256), I32),
            pltpu.VMEM((NQ, 4, 2, 4, 16, 1), F32),
            pltpu.VMEM((32, 16, 1), F32),
            pltpu.VMEM((128, 512), BF16),
            pltpu.VMEM((512, 256), BF16),
            pltpu.VMEM((NQ, 4, 256, 128), F32),
            pltpu.VMEM((NQ, 4, 256, 128), F32),
            pltpu.VMEM((NQ, 4, 72, 128), F32),
            pltpu.VMEM((NQ, 4, 72, 128), F32),
            pltpu.VMEM((NQ, NP - 1, 4, 64, 128), F32),
            pltpu.VMEM((NQ, NP - 1, 4, 64, 128), F32),
            pltpu.VMEM((NQ * 16, 2, 16, 128), F32),
            pltpu.VMEM((NQ * 16, 2, 16, 128), F32),
            pltpu.VMEM((NQ, 1, 128), F32),
            pltpu.VMEM((NQ * 16, 1, 128), F32),
            pltpu.VMEM((8, 128), F32),
            pltpu.VMEM((8, 8, 128), F32),
            dma,
            dma,
            dma((NQ,)),
            dma((2,)),
            dma((NQ, NP)),
            dma,
            dma((NQ,)),
            dma,
            dma((NQ,)),
            dma,
            dma,
            pltpu.SemaphoreType.REGULAR((2,)),
        ],
        compiler_params=pltpu.CompilerParams(
            collective_id=0, has_side_effects=True, vmem_limit_bytes=56_000_000
        ),
    )(counts, ids)
    return merged, terms


def solution(mesh):
    return jax.shard_map(
        shards,
        mesh=mesh,
        in_specs=(P("blk", "col"), P()),
        out_specs=(P("blk", "col"), P("blk")),
        check_vma=False,
    )
```
